32 devices in a mesh: dp: 4 (over y, x), fsdp: 8 (over z, core).
Axes of the slice: x: 2, y: 2, z: 4, core: 2. Of those that a mesh axis runs over, the one named last changes fastest.
Arguments:
- tokens: bfloat16 [32768, 768], P(('dp', 'fsdp')), may hold values from -6 to 6
- cotangent: bfloat16 [32768, 768], P(('dp', 'fsdp')), may hold values from -6 to 6
- lengths: int32 [64], P(('dp', 'fsdp')), may hold values from 128 to 512, as said below
- mb_count: int32 [4], replicated, may hold values from 1 to 2, as said below
- query_weight: bfloat16 [768, 768], P('fsdp'), may hold values from -0.21875 to 0.21875
- query_bias: bfloat16 [768], P('fsdp'), may hold values from -1.5 to 1.5
- key_weight: bfloat16 [768, 768], P('fsdp'), may hold values from -0.21875 to 0.21875
- value_weight: bfloat16 [768, 768], P('fsdp'), may hold values from -0.21875 to 0.21875
- value_bias: bfloat16 [768], P('fsdp'), may hold values from -1.5 to 1.5
- output_weight: bfloat16 [768, 768], P('fsdp'), may hold values from -1.75 to 1.75
- output_bias: bfloat16 [768], P('fsdp'), may hold values from -1.5 to 1.5
- first_gain: bfloat16 [768], P('fsdp'), may hold values from 0.5 to 1.5
- first_shift: bfloat16 [768], P('fsdp'), may hold values from -1.5 to 1.5
- up_weight: bfloat16 [768, 3072], P('fsdp'), may hold values from -0.21875 to 0.21875
- up_bias: bfloat16 [3072], P('fsdp'), may hold values from -1.5 to 1.5
- down_weight: bfloat16 [3072, 768], P('fsdp'), may hold values from -0.109375 to 0.109375
- down_bias: bfloat16 [768], P('fsdp'), may hold values from -1.5 to 1.5
- second_gain: bfloat16 [768], P('fsdp'), may hold values from 0.5 to 1.5
- second_shift: bfloat16 [768], P('fsdp'), may hold values from -1.5 to 1.5
Outputs:
- layer_out: bfloat16 [32768, 768], P(('dp', 'fsdp'))
- tokens_grad: bfloat16 [32768, 768], P(('dp', 'fsdp'))
- query_weight_grad: float32 [768, 768], P('fsdp')
- query_bias_grad: float32 [768], P('fsdp')
- key_weight_grad: float32 [768, 768], P('fsdp')
- value_weight_grad: float32 [768, 768], P('fsdp')
- value_bias_grad: float32 [768], P('fsdp')
- output_weight_grad: float32 [768, 768], P('fsdp')
- output_bias_grad: float32 [768], P('fsdp')
- first_gain_grad: float32 [768], P('fsdp')
- first_shift_grad: float32 [768], P('fsdp')
- up_weight_grad: float32 [768, 3072], P('fsdp')
- up_bias_grad: float32 [3072], P('fsdp')
- down_weight_grad: float32 [3072, 768], P('fsdp')
- down_bias_grad: float32 [768], P('fsdp')
- second_gain_grad: float32 [768], P('fsdp')
- second_shift_grad: float32 [768], P('fsdp')
The draws below stay inside these ranges and needn't reach their ends.
Inputs may be any that keep to these rules, and one draw needn't show every extreme that they name: `lengths`: keys at positions at or past a sequence's length are padding; some sequence has all 512 keys valid and some has 128. Data group g runs slots 0 .. mb_count[g] - 1 of each of its devices; some group runs all 2 and some runs one.
All inputs are finite; a program needn't handle non-finite values.
Results may differ from the reference program's by a relative error of at most 0.02.
Values may be sent and summed in bfloat16 or wider, within the bound.
A program may use at most 144 MiB of HBM per device.

```python
import math
import jax
import jax.numpy as jnp
from jax import lax

D = 768
HEADS = 12
HD = 64
FF = 3072
SEQ = 512
MB_CAP = 2
SEQ_MB = 1
SEQS = 64
TOKENS = 32768
N_DP = 4
N_FSDP = 8


def draw_lengths(key, part):
    values = jax.random.randint(jax.random.fold_in(key, 11), (SEQS,), SEQ // 4, SEQ + 1, dtype=jnp.int32)
    chosen = jax.random.permutation(jax.random.fold_in(key, 12), SEQS)
    values = values.at[chosen[0]].set(SEQ)
    values = values.at[chosen[1]].set(SEQ // 4)
    return values


def draw_mb_count(key, part):
    values = jax.random.randint(jax.random.fold_in(key, 21), (N_DP,), 1, MB_CAP + 1, dtype=jnp.int32)
    chosen = jax.random.permutation(jax.random.fold_in(key, 22), N_DP)
    values = values.at[chosen[0]].set(MB_CAP)
    values = values.at[chosen[1]].set(1)
    return values


def with_spikes(values, own_key, source, target, parts, factor):
    def block_of(dim):
        return (jnp.arange(values.shape[dim]) // (values.shape[dim] // parts)).reshape((-1,) + (1,) * (values.ndim - 1 - dim))

    one_side = jax.random.permutation(own_key, parts)[block_of(target)]
    second = (block_of(target) + parts // 2) % parts
    return jnp.where((block_of(source) == one_side) | (block_of(source) == second), factor * values, values)


def block_scale(stream_key, shape, pieces, least, high):
    def one(dim, parts):
        heights = jax.random.uniform(jax.random.fold_in(jax.random.fold_in(stream_key, 6), dim), (parts,), jnp.float32, least / len(pieces), high / len(pieces))
        return jnp.repeat(jnp.exp(heights), shape[dim] // parts).reshape((-1,) + (1,) * (len(shape) - dim - 1))

    level = one(*pieces[0])
    for cut in pieces[1:]:
        level = level * one(*cut)
    return level


def scatter_about(rng, extent, deviation, most, shards=(), held_as=jnp.bfloat16):
    entries = deviation * jax.random.normal(rng, extent, jnp.float32)
    if shards:
        entries = entries * block_scale(rng, extent, shards, -0.22, 0.18)
    return jnp.clip(entries, -most, most).astype(held_as)


def gaussian_with(rng, dims, deviation, reach, cuts, heavy, held_as=jnp.bfloat16):
    values = deviation * jax.random.normal(rng, dims, jnp.float32)
    if cuts:
        values = values * block_scale(rng, dims, cuts, -0.22, 0.18)
    return jnp.clip(with_spikes(values, jax.random.fold_in(rng, 3), *heavy), -reach, reach).astype(held_as)


def setup_inputs(seed: int = 0) -> dict:
    splits = jax.random.split(jax.random.key(seed), 20)
    return {
        "tokens": scatter_about(splits[0], (TOKENS, D), 1.0, 6.0, ((0, 32),)),
        "cotangent": gaussian_with(splits[1], (TOKENS, D), 1.0, 6.0, ((0, 32),), (0, 1, 32, 2.75)),
        "lengths": draw_lengths(jax.random.fold_in(splits[19], 71), 0),
        "mb_count": draw_mb_count(jax.random.fold_in(splits[19], 71), 0),
        "query_weight": scatter_about(splits[4], (D, D), D ** -0.5, 0.21875, ((0, 8),)),
        "query_bias": scatter_about(splits[5], (D,), 0.3, 1.5, ((0, 8),)),
        "key_weight": scatter_about(splits[6], (D, D), D ** -0.5, 0.21875, ((0, 8),)),
        "value_weight": scatter_about(splits[7], (D, D), D ** -0.5, 0.21875, ((0, 8),)),
        "value_bias": scatter_about(splits[8], (D,), 0.3, 1.5, ((0, 8),)),
        "output_weight": scatter_about(splits[9], (D, D), (D // 64) ** -0.5, 1.75, ((0, 8),)),
        "output_bias": scatter_about(splits[10], (D,), 0.3, 1.5, ((0, 8),)),
        "first_gain": jnp.clip(1.0 + 0.1 * jax.random.normal(splits[11], (D,), jnp.float32), 0.5, 1.5).astype(jnp.bfloat16),
        "first_shift": scatter_about(splits[12], (D,), 0.3, 1.5, ((0, 8),)),
        "up_weight": scatter_about(splits[13], (D, FF), D ** -0.5, 0.21875, ((0, 8),)),
        "up_bias": scatter_about(splits[14], (FF,), 0.3, 1.5, ((0, 8),)),
        "down_weight": scatter_about(splits[15], (FF, D), FF ** -0.5, 0.109375, ((0, 8),)),
        "down_bias": scatter_about(splits[16], (D,), 0.3, 1.5, ((0, 8),)),
        "second_gain": jnp.clip(1.0 + 0.1 * jax.random.normal(splits[17], (D,), jnp.float32), 0.5, 1.5).astype(jnp.bfloat16),
        "second_shift": scatter_about(splits[18], (D,), 0.3, 1.5, ((0, 8),)),
    }


@jax.custom_vjp
def low(v):
    return lax.optimization_barrier(v.astype(jnp.bfloat16)).astype(jnp.float32)

@jax.custom_vjp
def low_back(v):
    return v

def low_keep(v):
    return (low(v), None)

def low_pass(kept, grad):
    return (grad,)

def back_keep(v):
    return (v, None)

def back_low(kept, grad):
    return (low(grad),)
low.defvjp(low_keep, low_pass)
low_back.defvjp(back_keep, back_low)

def matmul(left, right):
    return jnp.dot(left, right, precision=lax.Precision.HIGHEST)

def layer_norm(hidden, gain, shift):
    centre = hidden - lax.optimization_barrier(jnp.mean(hidden, axis=-1, keepdims=True))
    inverse = lax.rsqrt(lax.optimization_barrier(jnp.mean(centre * centre, axis=-1, keepdims=True)) + 1e-05)
    return centre * inverse * gain + shift

def attend(item):
    query_heads, key_heads, value_heads, length = item
    scores = jnp.einsum('qhd,khd->hqk', query_heads, key_heads, precision=lax.Precision.HIGHEST) * HD ** (-0.5)
    scores = low_back(scores)
    visible = jnp.arange(SEQ, dtype=jnp.int32) < length
    scores = jnp.where(visible[None, None, :], scores, -1000000000.0)
    probs = low(jax.nn.softmax(scores, axis=-1))
    return jnp.einsum('hqk,khd->qhd', probs, value_heads, precision=lax.Precision.HIGHEST)

def layer(inputs, seq_lengths, params):
    w_query, b_query, w_key, w_value, b_value, w_output, b_output, gain_one, shift_one, w_up, b_up, w_down, b_down, gain_two, shift_two = params
    count = inputs.shape[0]
    flat = inputs.reshape(-1, D)
    queries = low_back(low(matmul(flat, w_query) + b_query))
    key_rows = low_back(low(matmul(flat, w_key)))
    value_rows = low_back(low(matmul(flat, w_value) + b_value))

    def split(values):
        return values.reshape(count, SEQ, HEADS, HD)
    context = lax.map(jax.checkpoint(attend), (split(queries), split(key_rows), split(value_rows), seq_lengths))
    context = low_back(low(context.reshape(-1, D)))
    branch = low_back(matmul(context, w_output) + b_output)
    middle = layer_norm(flat + branch, gain_one, shift_one)
    upper = low_back(matmul(low(middle), w_up) + b_up)
    active = low(jax.nn.gelu(upper, approximate=False))
    down = low_back(matmul(active, w_down) + b_down)
    result = layer_norm(middle + down, gain_two, shift_two)
    return result.reshape(inputs.shape)

def reference(tokens, cotangent, lengths, mb_count, query_weight, query_bias, key_weight, value_weight, value_bias, output_weight, output_bias, first_gain, first_shift, up_weight, up_bias, down_weight, down_bias, second_gain, second_shift):
    params = tuple((item.astype(jnp.float32) for item in (query_weight, query_bias, key_weight, value_weight, value_bias, output_weight, output_bias, first_gain, first_shift, up_weight, up_bias, down_weight, down_bias, second_gain, second_shift)))
    seq_total = tokens.shape[0] // SEQ
    per_device = MB_CAP * SEQ_MB
    seq_ids = jnp.arange(seq_total, dtype=jnp.int32)
    group_ids = seq_ids // per_device // N_FSDP
    slot_ids = seq_ids % per_device // SEQ_MB
    valid = (slot_ids < mb_count[group_ids]).astype(jnp.float32)
    inputs_all = tokens.astype(jnp.float32).reshape(seq_total, SEQ, D)
    grads_all = cotangent.astype(jnp.float32).reshape(seq_total, SEQ, D) * valid[:, None, None]
    block = math.gcd(seq_total, max(1, 4096 // SEQ))
    blocks = seq_total // block
    inputs_all = inputs_all.reshape(blocks, block, SEQ, D)
    grads_all = grads_all.reshape(blocks, block, SEQ, D)
    lengths_all = lengths.reshape(blocks, block)

    def step(totals, item):
        inputs_block, grad_block, length_block = item

        def forward(values, *weights):
            return layer(values, length_block, weights)
        result, pull = jax.vjp(forward, inputs_block, *params)
        pulled = pull(grad_block)
        totals = tuple((total + piece for total, piece in zip(totals, pulled[1:])))
        return (totals, (result.astype(jnp.bfloat16), pulled[0].astype(jnp.bfloat16)))
    start = tuple((jnp.zeros(item.shape, jnp.float32) for item in params))
    totals, (results, input_grads) = lax.scan(step, start, (inputs_all, grads_all, lengths_all))
    return (results.reshape(-1, D), input_grads.reshape(-1, D), totals[0], totals[1], totals[2], totals[3], totals[4], totals[5], totals[6], totals[7], totals[8], totals[9], totals[10], totals[11], totals[12], totals[13], totals[14])
```

```python
import jax
import jax.numpy as jnp
from jax import lax
from jax.experimental import pallas as pl
from jax.experimental.pallas import tpu as pltpu
from jax.sharding import PartitionSpec as P

HEADS = 12
MB_CAP = 2
EPSILON = 1e-05
TILE = 256
BF = jnp.bfloat16
F32 = jnp.float32


def dot(a, b):
    return jnp.dot(a, b, preferred_element_type=F32)


def dot_t(a, b):
    return lax.dot_general(a, b, (((1,), (1,)), ((), ())), preferred_element_type=F32)


def t_dot(a, b):
    return lax.dot_general(a, b, (((0,), (0,)), ((), ())), preferred_element_type=F32)


def fold(x):
    return jnp.sum(x.reshape(x.shape[0] // 8, 8, x.shape[1]), axis=0)


def rows_of(i, size=TILE):
    return pl.ds(pl.multiple_of(i * size, size), size)


def lanes_of(i, size=128):
    return pl.ds(pl.multiple_of(i * size, size), size)


def split3(x):
    hi = x.astype(BF).astype(F32)
    mid = (x - hi).astype(BF).astype(F32)
    return hi, mid, x - hi - mid


class Body:
    def __init__(self, **refs):
        self.__dict__.update(refs)
        self.rows, self.width = self.tok.shape
        self.seqs = self.lens.shape[0]
        self.seq = self.rows // self.seqs
        self.pairs = self.width // 128
        self.ff_blocks = self.w_up.shape[0]
        self.tiles = self.rows // TILE
        self.factor = 64**-0.5
        self.base = self.factor * 1.4426950408889634

    def vec(self, i):
        return self.vectors[i : i + 1, :]

    def add_sum(self, slot, x, lanes=None):
        lanes = slice(None) if lanes is None else lanes
        self.sums[slot, :, lanes] += fold(x)

    def masks(self):
        lane = lax.broadcasted_iota(jnp.int32, (1, 128), 1)
        first = jnp.where(lane < 64, 1.0, 0.0)
        return (first.astype(BF), (1.0 - first).astype(BF)), lane

    def prepare(self):
        self.sums[...] = jnp.zeros_like(self.sums)
        self.lse[...] = jnp.zeros_like(self.lse)
        lane = lax.broadcasted_iota(jnp.int32, (self.seq, 128), 1)
        pos = lax.broadcasted_iota(jnp.int32, (self.seq, 128), 0)
        for s in range(self.seqs):
            hidden = jnp.where(pos < self.lens[s], 0.0, -1e9)
            for h in range(2):
                base = 64 * (1 - h)
                ext = jnp.where(lane == base, hidden, 0.0)
                ext = jnp.where((lane > base) & (lane < base + 4), 1.0, ext)
                self.key_ext[s, h] = ext.astype(BF)

    def qkv_tile(self, i):
        x = self.tok[rows_of(i), :]
        self.q[rows_of(i), :] = (dot(x, self.w_q[...]) + self.vec(0)).astype(BF)
        self.k[rows_of(i), :] = dot(x, self.w_k[...]).astype(BF)
        self.v[rows_of(i), :] = (dot(x, self.w_v[...]) + self.vec(1)).astype(BF)

    def attend(self, n):
        s, p = n // self.pairs, n % self.pairs
        masks, lane = self.masks()
        lanes = lanes_of(p)
        k, v = self.k[rows_of(s, self.seq), lanes], self.v[rows_of(s, self.seq), lanes]
        ones = jnp.ones((self.seq, 128), BF)
        chunk = min(TILE, self.seq)
        keys = [k * masks[h] + self.key_ext[s, h] for h in range(2)]
        vals = [jnp.concatenate([v * masks[h], ones * masks[h]], axis=1) for h in range(2)]
        for c in range(self.seq // chunk):
            rows = pl.ds(pl.multiple_of(s * self.seq + c * chunk, chunk), chunk)
            q = self.q[rows, lanes]
            acc, tops = 0.0, []
            for h in range(2):
                one = jnp.where(lane == 64 * (1 - h), 1.0, 0.0).astype(BF)
                scores = dot_t(q * masks[h] + one, keys[h]) * self.base
                top = jnp.max(scores, axis=-1, keepdims=True)
                acc = acc + dot(jnp.exp2(scores - top).astype(BF), vals[h])
                tops.append(top)
            total = acc[:, 128:]
            self.ctx[rows, lanes] = (acc[:, :128] / total).astype(BF)
            lse = jnp.where(lane < 64, tops[0], tops[1]) + jnp.log2(total)
            old = self.lse[rows, :]
            old = jnp.where(lane == 2 * p, lse[:, :1], old)
            self.lse[rows, :] = jnp.where(lane == 2 * p + 1, lse[:, 64:65], old)

    def first_norm(self, i):
        r = rows_of(i)
        x = self.tok[r, :].astype(F32) + dot(self.ctx[r, :], self.w_o[...]) + self.vec(2)
        x = x - jnp.mean(x, axis=-1, keepdims=True)
        inverse = lax.rsqrt(jnp.mean(x * x, axis=-1, keepdims=True) + EPSILON)
        normed = x * inverse
        mid = normed * self.vec(3) + self.vec(4)
        self.inv1[r, :] = jnp.broadcast_to(inverse, (TILE, 128))
        self.normed1[r, :] = normed.astype(BF)
        self.mid[r, :] = mid.astype(BF)
        self.gs[r, :] = mid + self.vec(5)

    def feed(self, j, i):
        r = rows_of(i)
        upper = dot(self.mid[r, :], self.w_up[j]) + self.vectors[pl.ds(8 + j, 1), :]
        cdf = 0.5 * lax.erf(upper * 0.7071067811865476) + 0.5
        self.active[j, r, :] = (upper * cdf).astype(BF)
        slope = cdf + upper * (0.3989422804014327 * jnp.exp2(upper * upper * -0.7213475204444817))
        self.slope[j, r, :] = slope.astype(BF)
        self.gs[r, :] += dot(self.active[j, r, :], self.w_down[j])

    def second_norm(self, i):
        r = rows_of(i)
        x = self.gs[r, :]
        x = x - jnp.mean(x, axis=-1, keepdims=True)
        inverse = lax.rsqrt(jnp.mean(x * x, axis=-1, keepdims=True) + EPSILON)
        normed = x * inverse
        keep = self.valid[(i * TILE) // (self.rows // MB_CAP)]
        g = self.cot[r, :].astype(F32) * keep
        self.out[r, :] = (normed * self.vec(6) + self.vec(7)).astype(BF)
        self.add_sum(6, g * normed)
        self.add_sum(7, g)
        e = g * self.vec(6)
        e = e - jnp.mean(e, axis=-1, keepdims=True) - normed * jnp.mean(e * normed, axis=-1, keepdims=True)
        e = e * inverse
        self.gs[r, :] = e
        low = e.astype(BF)
        self.gd[r, :] = low
        self.add_sum(5, low.astype(F32))

    def feed_back(self, j, i):
        r = rows_of(i)
        gu = (dot_t(self.gd[r, :], self.w_down[j]) * self.slope[j, r, :].astype(F32)).astype(BF)
        self.slope[j, r, :] = gu
        self.sums[pl.ds(8 + j, 1)] += fold(gu.astype(F32))[None]
        self.gs[r, :] += dot_t(gu, self.w_up[j])

    def feed_grads(self, j, i):
        r = rows_of(i)
        lanes = lanes_of(i, TILE)
        self.w_down[j, r, :] = t_dot(self.active[j, :, lanes], self.gd[...]).astype(BF)
        self.w_up[j, r, :] = t_dot(self.mid[:, lanes], self.slope[j]).astype(BF)

    def first_back(self, i):
        r = rows_of(i)
        g = self.gs[r, :]
        normed = self.normed1[r, :].astype(F32)
        self.add_sum(3, g * normed)
        self.add_sum(4, g)
        e = g * self.vec(3)
        e = e - jnp.mean(e, axis=-1, keepdims=True) - normed * jnp.mean(e * normed, axis=-1, keepdims=True)
        e = e * self.inv1[r, :1]
        self.gs[r, :] = e
        low = e.astype(BF)
        self.gd[r, :] = low
        self.add_sum(2, low.astype(F32))
        self.gctx[r, :] = dot_t(low, self.w_o[...]).astype(BF)

    def out_grad(self, i):
        self.w_o[rows_of(i), :] = t_dot(self.ctx[:, lanes_of(i, TILE)], self.gd[...]).astype(BF)

    def attend_back(self, n):
        s, p = n // self.pairs, n % self.pairs
        masks, lane = self.masks()
        lanes = lanes_of(p)
        rows = rows_of(s, self.seq)
        q, k, v = self.q[rows, lanes], self.k[rows, lanes], self.v[rows, lanes]
        go = self.gctx[rows, lanes]
        prod = go.astype(F32) * self.ctx[rows, lanes].astype(F32)
        lse = self.lse[rows, :]
        chunk = min(TILE, self.seq)
        gq = 0.0
        gks, gvs = [0.0] * (self.seq // chunk), [0.0] * (self.seq // chunk)
        for h in range(2):
            b = 64 * (1 - h)

            def ext(column, one):
                parts = split3(column)
                e = jnp.where(lane == b, one, 0.0)
                for x in range(3):
                    e = jnp.where(lane == b + 1 + x, parts[x], e)
                return e.astype(BF)

            delta = jnp.sum(prod * masks[h].astype(F32), axis=-1, keepdims=True)
            level = jnp.sum(jnp.where(lane == 2 * p + h, lse, 0.0), axis=-1, keepdims=True)
            qh, kh, gh = q * masks[h], k * masks[h], go * masks[h]
            q_ext = qh + ext(level * (-1.0 / self.base), 1.0)
            g_ext = gh + ext(-delta, 0.0)
            k_ext = kh + self.key_ext[s, h]
            v_ext = v * masks[h] + self.key_ext[s, h]
            for c in range(self.seq // chunk):
                part = slice(c * chunk, (c + 1) * chunk)
                probs = jnp.exp2(dot_t(k_ext[part], q_ext) * self.base)
                gs = (probs * dot_t(v_ext[part], g_ext)).astype(BF)
                gvs[c] = gvs[c] + dot(probs.astype(BF), gh)
                gks[c] = gks[c] + dot(gs, qh)
                gq = gq + t_dot(gs, kh[part])
        gq = (gq * self.factor).astype(BF)
        self.q[rows, lanes] = gq
        self.add_sum(0, gq.astype(F32), lanes)
        for c in range(self.seq // chunk):
            r = pl.ds(pl.multiple_of(s * self.seq + c * chunk, chunk), chunk)
            self.k[r, lanes] = (gks[c] * self.factor).astype(BF)
            gv = gvs[c].astype(BF)
            self.v[r, lanes] = gv
            self.add_sum(1, gv.astype(F32), lanes)

    def qkv_grads(self, i):
        x = self.tok[:, lanes_of(i, TILE)].T
        r = rows_of(i)
        for m, g in enumerate((self.q, self.k, self.v)):
            self.g_qkv[m, r, :] = dot(x, g[...]).astype(BF)

    def tokens_grad(self, i):
        r = rows_of(i)
        g = self.gs[r, :] + dot_t(self.q[r, :], self.w_q[...])
        g = g + dot_t(self.k[r, :], self.w_k[...]) + dot_t(self.v[r, :], self.w_v[...])
        self.gtok[r, :] = g.astype(BF)


def loop(n, f):
    lax.fori_loop(0, n, lambda i, c: (f(i), c)[1], 0)


def layer_kernel(
    lens, valid, tok_hbm, cot_hbm, vectors, wq_h, wk_h, wv_h, wo_h, up_h, down_h,
    out_hbm, gtok_hbm, gq_h, gk_h, gv_h, go_h, gup_h, gdown_h, sums_out,
    tok, cot, w_q, w_k, w_v, w_o, w_up, w_down, q, k, v, ctx, normed1, inv1, mid, active, slope,
    gs, gd, lse, key_ext, g_qkv, sums, sems,
):
    copies = [pltpu.make_async_copy(a, b, sems.at[i]) for i, (a, b) in enumerate(
        ((tok_hbm, tok), (wq_h, w_q), (wk_h, w_k), (wv_h, w_v), (wo_h, w_o)))]
    blocks = w_up.shape[0]
    width = tok.shape[1]
    for j in range(blocks):
        copies.append(pltpu.make_async_copy(up_h.at[:, j * width : (j + 1) * width], w_up.at[j], sems.at[5 + j]))
        copies.append(pltpu.make_async_copy(down_h.at[j * width : (j + 1) * width], w_down.at[j], sems.at[9 + j]))
    copies.append(pltpu.make_async_copy(cot_hbm, cot, sems.at[13]))
    for c in copies:
        c.start()
    b = Body(
        lens=lens, valid=valid, tok=tok, cot=cot, vectors=vectors, w_q=w_q, w_k=w_k, w_v=w_v, w_o=w_o,
        w_up=w_up, w_down=w_down, q=q, k=k, v=v, ctx=ctx, normed1=normed1, inv1=inv1, mid=mid, active=active,
        slope=slope, gs=gs, gd=gd, lse=lse, key_ext=key_ext, g_qkv=g_qkv, sums=sums, out=cot, gctx=cot, gtok=tok,
    )
    b.prepare()
    for c in copies[:4]:
        c.wait()
    loop(b.tiles, b.qkv_tile)
    loop(b.seqs * b.pairs, b.attend)
    for c in copies[4:]:
        c.wait()
    loop(b.tiles, b.first_norm)
    loop(blocks * b.tiles, lambda n: b.feed(n // b.tiles, n % b.tiles))
    loop(b.tiles, b.second_norm)
    done = pltpu.make_async_copy(cot, out_hbm, sems.at[0])
    done.start()

    def block(j):
        loop(b.tiles, lambda i: b.feed_back(j, i))
        loop(width // TILE, lambda i: b.feed_grads(j, i))

    loop(blocks, block)
    done.wait()
    loop(b.tiles, b.first_back)
    loop(width // TILE, b.out_grad)
    loop(b.seqs * b.pairs, b.attend_back)
    loop(width // TILE, b.qkv_grads)
    loop(b.tiles, b.tokens_grad)
    sums_out[...] = jnp.sum(sums[...], axis=1)
    outs = [(tok, gtok_hbm), (w_o, go_h), (g_qkv.at[0], gq_h), (g_qkv.at[1], gk_h), (g_qkv.at[2], gv_h)]
    for j in range(blocks):
        outs.append((w_up.at[j], gup_h.at[:, j * width : (j + 1) * width]))
        outs.append((w_down.at[j], gdown_h.at[j * width : (j + 1) * width]))
    copies = [pltpu.make_async_copy(a, o, sems.at[i]) for i, (a, o) in enumerate(outs)]
    for c in copies:
        c.start()
    for c in copies:
        c.wait()


def layer(lens, valid, tok, cot, vectors, w_q, w_k, w_v, w_o, w_up, w_down):
    rows, width = tok.shape
    seqs = lens.shape[0]
    seq = rows // seqs
    ff = w_up.shape[1]
    blocks = ff // width
    any_spec = pl.BlockSpec(memory_space=pl.ANY)
    vm = pl.BlockSpec(memory_space=pltpu.VMEM)
    sm = pl.BlockSpec(memory_space=pltpu.SMEM)
    square = pltpu.VMEM((width, width), BF)
    act = pltpu.VMEM((rows, width), BF)
    shape = jax.ShapeDtypeStruct
    sq = shape((width, width), BF)
    return pl.pallas_call(
        layer_kernel,
        out_shape=(shape(tok.shape, BF), shape(tok.shape, BF), sq, sq, sq, sq,
                   shape(w_up.shape, BF), shape(w_down.shape, BF), shape((16, width), F32)),
        in_specs=[sm, sm, any_spec, any_spec, vm] + [any_spec] * 6,
        out_specs=(any_spec,) * 8 + (vm,),
        scratch_shapes=[
            act, act, square, square, square, square,
            pltpu.VMEM((blocks, width, width), BF), pltpu.VMEM((blocks, width, width), BF),
            act, act, act, act, act, pltpu.VMEM((rows, 128), F32), act,
            pltpu.VMEM((blocks, rows, width), BF), pltpu.VMEM((blocks, rows, width), BF),
            pltpu.VMEM((rows, width), F32), act, pltpu.VMEM((rows, 128), F32),
            pltpu.VMEM((seqs, 2, seq, 128), BF), pltpu.VMEM((3, width, width), BF),
            pltpu.VMEM((16, 8, width), F32), pltpu.SemaphoreType.DMA((16,)),
        ],
        compiler_params=pltpu.CompilerParams(vmem_limit_bytes=67043328),
    )(lens, valid, tok, cot, vectors, w_q, w_k, w_v, w_o, w_up, w_down)


def local(tokens, cotangent, lengths, mb_count, query_weight, query_bias, key_weight, value_weight, value_bias,
          output_weight, output_bias, first_gain, first_shift, up_weight, up_bias, down_weight, down_bias,
          second_gain, second_shift):
    width = tokens.shape[1]
    group_count = mb_count[lax.axis_index("dp")]
    valid = (jnp.arange(MB_CAP, dtype=jnp.int32) < group_count).astype(F32)

    def gather(x):
        return lax.all_gather(x, "fsdp", axis=0, tiled=True)

    small = (query_bias, value_bias, output_bias, first_gain, first_shift, down_bias, second_gain, second_shift)
    packed = gather(jnp.stack(small, axis=1))
    ups = gather(up_bias).reshape(-1, width)
    vectors = jnp.concatenate([packed.T, ups, jnp.zeros((8 - ups.shape[0], width), BF)], axis=0).astype(F32)
    weights = [gather(w) for w in (query_weight, key_weight, value_weight, output_weight, up_weight, down_weight)]
    res = layer(lengths, valid, tokens, cotangent, vectors, *weights)
    out, gtok, grads, sums = res[0], res[1], res[2:8], res[8]

    def reduce(x):
        y = lax.psum_scatter(x, "fsdp", scatter_dimension=0, tiled=True)
        return lax.psum(y, "dp").astype(F32)

    gq, gk, gv, go, gup, gdown = [reduce(g) for g in grads]
    total = lax.psum(sums, ("dp", "fsdp"))
    here = lax.axis_index("fsdp")

    def piece(x, n):
        return lax.dynamic_slice_in_dim(x, here * n, n, 0)

    part = [piece(total[i], query_bias.shape[0]) for i in range(8)]
    up_part = piece(total[8 : 8 + ups.shape[0]].reshape(-1), up_bias.shape[0])
    return (out, gtok, gq, part[0], gk, gv, part[1], go, part[2], part[3], part[4], gup, up_part, gdown,
            part[5], part[6], part[7])


def solution(mesh):
    row, shard, vector = P(("dp", "fsdp"), None), P("fsdp", None), P("fsdp")
    return jax.shard_map(
        local,
        mesh=mesh,
        in_specs=(row, row, P(("dp", "fsdp")), P(), shard, vector, shard, shard, vector, shard, vector, vector,
                  vector, shard, vector, shard, vector, vector, vector),
        out_specs=(row, row, shard, vector, shard, shard, vector, shard, vector, vector, vector, shard, vector,
                   shard, vector, vector, vector),
        check_vma=False,
    )
```
